8 devices in a mesh: dp: 2 (over z, y), row: 2 (over x), fsdp: 2 (over core).
Axes of the slice: x: 2, y: 2, z: 1, core: 2. Of those that a mesh axis runs over, the one named last changes fastest.
Arguments:
- x_saved: bfloat16 [2, 16384, 896], P(None, ('dp', 'row', 'fsdp'))
- dy_out: bfloat16 [2, 16384, 896], P(None, ('dp', 'row', 'fsdp'))
- w_gate: bfloat16 [896, 4864], P(None, ('row', 'fsdp'))
- w_up: bfloat16 [896, 4864], P(None, ('row', 'fsdp'))
- w_down: bfloat16 [4864, 896], P(('row', 'fsdp'))
- g_next: float32 [8, 3, 896, 4864], P(('dp', 'row', 'fsdp'))
Outputs:
- output 1: bfloat16 [2, 16384, 896], P(None, ('dp', 'row', 'fsdp'))
- output 2: float32 [3, 896, 4864], P(None, None, ('row', 'fsdp'))
- output 3: float32 [8, 3, 896, 4864], P(('dp', 'row', 'fsdp'))
All inputs are finite; a program needn't handle non-finite values.
Results may differ from the reference program's by a relative error of at most 0.00911364.
Values are sent between devices in bfloat16 or wider.
A program may use at most 1 GiB of HBM per device.

```python
import jax
import jax.numpy as jnp
from jax import lax

DEVICES = 8
TOK_DEV = 2048
D_MODEL = 896
FF_DIM = 4864
MICRO_COUNT = 2


def setup_inputs(seed: int = 0) -> dict:
    key_list = jax.random.split(jax.random.key(seed), 6)
    tok_all = DEVICES * TOK_DEV
    act_shape = (MICRO_COUNT, tok_all, D_MODEL)
    x_saved = jax.random.normal(key_list[0], act_shape, jnp.float32)
    dy_out = jax.random.normal(key_list[1], act_shape, jnp.float32)
    w_gate = jax.random.normal(key_list[2], (D_MODEL, FF_DIM), jnp.float32) * D_MODEL ** -0.5
    w_up = jax.random.normal(key_list[3], (D_MODEL, FF_DIM), jnp.float32) * D_MODEL ** -0.5
    w_down = jax.random.normal(key_list[4], (FF_DIM, D_MODEL), jnp.float32) * FF_DIM ** -0.5
    g_next = jax.random.normal(key_list[5], (DEVICES, 3, D_MODEL, FF_DIM), jnp.float32) * DEVICES ** -0.5
    return {"x_saved": x_saved.astype(jnp.bfloat16), "dy_out": dy_out.astype(jnp.bfloat16), "w_gate": w_gate.astype(jnp.bfloat16), "w_up": w_up.astype(jnp.bfloat16), "w_down": w_down.astype(jnp.bfloat16), "g_next": g_next}


def silu_slope(pre_act):
    sigmoid_val = jax.nn.sigmoid(pre_act)
    return sigmoid_val * (1.0 + pre_act * (1.0 - sigmoid_val))


def device_backward(x_dev, dy_dev, w_gate, w_up, w_down):
    def one_micro(grad_acc, micro_pair):
        x_mb, dy_mb = micro_pair
        pre_gate = jnp.dot(x_mb, w_gate, preferred_element_type=jnp.float32)
        pre_up = jnp.dot(x_mb, w_up, preferred_element_type=jnp.float32)
        act_gate = jax.nn.silu(pre_gate)
        hidden = (act_gate * pre_up).astype(jnp.bfloat16)
        d_hidden = jnp.dot(dy_mb, w_down.T, preferred_element_type=jnp.float32)
        d_gate = (d_hidden * pre_up * silu_slope(pre_gate)).astype(jnp.bfloat16)
        d_up = (d_hidden * act_gate).astype(jnp.bfloat16)
        dx_mb = (jnp.dot(d_gate, w_gate.T, preferred_element_type=jnp.float32) + jnp.dot(d_up, w_up.T, preferred_element_type=jnp.float32)).astype(jnp.bfloat16)
        grad_mb = jnp.stack([
            jnp.dot(x_mb.T, d_gate, preferred_element_type=jnp.float32),
            jnp.dot(x_mb.T, d_up, preferred_element_type=jnp.float32),
            jnp.dot(dy_mb.T, hidden, preferred_element_type=jnp.float32),
        ])
        return grad_acc + grad_mb, dx_mb

    grad_init = jnp.zeros((3, D_MODEL, FF_DIM), jnp.float32)
    grad_sum, dx_dev = lax.scan(one_micro, grad_init, (x_dev, dy_dev))
    return dx_dev, grad_sum


def reference(x_saved, dy_out, w_gate, w_up, w_down, g_next):
    x_dev = x_saved.reshape(MICRO_COUNT, DEVICES, TOK_DEV, D_MODEL).transpose(1, 0, 2, 3)
    dy_dev = dy_out.reshape(MICRO_COUNT, DEVICES, TOK_DEV, D_MODEL).transpose(1, 0, 2, 3)

    def per_device(dev_pair):
        return device_backward(dev_pair[0], dev_pair[1], w_gate, w_up, w_down)

    dx_dev, grad_layer = lax.map(per_device, (x_dev, dy_dev))
    dx_out = dx_dev.transpose(1, 0, 2, 3).reshape(MICRO_COUNT, DEVICES * TOK_DEV, D_MODEL)
    grad_next = jnp.sum(g_next.astype(jnp.bfloat16).astype(jnp.float32), axis=0)
    return dx_out, grad_next, grad_layer
```

```python
import jax
import jax.numpy as jnp
from jax import lax
from jax.experimental import pallas as pl
from jax.experimental.pallas import tpu as pltpu
from jax.sharding import PartitionSpec as P

TOK_AXES = ("dp", "row", "fsdp")
GROUP_AXES = ("row", "fsdp")

D = 896
FF = 4864
N = 4096
SH = FF // 4
FT = 256
T = 1024
NF = FF // FT
C = N // T
XB = 512
UN = 42
UR, UC = 128, 640
A0, B0, C0, D0 = 9, 12, 18, 24
PS, QS = C0 - B0 + 1, D0 - C0 + 1
NT = (((1,), (1,)), ((), ()))
F32, BF16 = jnp.float32, jnp.bfloat16
MESH = pl.DeviceIdType.MESH


def step_kernel(x_h, dy_h, w1_h, w3_h, w2_h, g_h,
                dw_h, dx_h, dn_h, wg1, wg3, wg2, ra_h, rx_h, ry_h,
                xt, dyt, acc, wb, wn, dwb, gba, gbb, ob,
                ga, gb_in, sa, ra, pb, rx, qb, ry, tb,
                wsem, dsem, xsem, osem, lsem, agl, ags, agr,
                gas, gbs, ras, rxs, rys, tbs, sas, sar, sxs, sxr, sys_, syr):
    d = lax.axis_index("dp")
    r = lax.axis_index("row")
    c = lax.axis_index("fsdp")
    core = (d, r, 1 - c)
    xnb = (d, 1 - r, c)
    ynb = (1 - d, r, c)
    s = 2 * r + c
    so = 2 * (1 - r) + c

    bar = pltpu.get_barrier_semaphore()
    for dev in (core, xnb, ynb):
        pl.semaphore_signal(bar, inc=1, device_id=dev, device_id_type=MESH)
    pl.semaphore_wait(bar, 3)

    own = (w1_h, w3_h, w2_h)
    full = (wg1, wg3, wg2)

    def rows(start, size):
        return pl.ds(pl.multiple_of(start, 32), size)

    def remote(src, dst, ssem, rsem, dev):
        return pltpu.make_async_remote_copy(src_ref=src, dst_ref=dst, send_sem=ssem, recv_sem=rsem, device_id=dev, device_id_type=MESH)

    H = SH // 2

    def ag(kind, w):
        if kind == 0:
            return remote(own[w], full[w].at[rows(s * SH, SH)], ags.at[kind, w], agr.at[kind, w], core)
        if kind == 1:
            return remote(own[w].at[rows(d * H, H)], full[w].at[rows(s * SH + d * H, H)], ags.at[kind, w], agr.at[kind, w], xnb)
        got = full[w].at[rows(so * SH + d * H, H)]
        if kind == 2:
            return remote(got, got, ags.at[kind, w], agr.at[kind, w], ynb)
        if kind == 3:
            return remote(got, got, ags.at[kind, w], agr.at[kind, w], core)
        got = full[w].at[rows(so * SH + (1 - d) * H, H)]
        return remote(got, got, ags.at[kind, w], agr.at[kind, w], core)

    for w in range(3):
        ag(1, w).start()
    for w in range(3):
        ag(0, w).start()

    def edge(w, e):
        off = e * (SH - 192)
        return pltpu.make_async_copy(own[w].at[rows(off, 192)], full[w].at[rows(s * SH + off, 192)], agl.at[w, e])

    for w in range(3):
        for e in range(2):
            edge(w, e).start()

    def tile(j):
        one = jnp.where(j < 4, 5 + j, jnp.where(j < 9, 8 - j, jnp.where(j < 13, 6 + j, 27 - j)))
        zero = j
        t = jnp.where(r == c, zero, one)
        return jnp.where(r == 1, NF - 1 - t, t)

    def wcopy(j, slot, mine):
        t = tile(j)
        out = []
        for w in range(3):
            if mine:
                src = own[w].at[rows(t * FT - s * SH, FT)]
            else:
                src = full[w].at[rows(t * FT, FT)]
            out.append(pltpu.make_async_copy(src, wb.at[slot, pl.ds(w * FT, FT)], wsem.at[slot, w]))
        return out

    for cp in wcopy(0, 0, True):
        cp.start()
    for cp in wcopy(1, 1, True):
        cp.start()

    nx = N // XB

    def xload(k, src):
        return pltpu.make_async_copy(src.at[pl.ds(pl.multiple_of(k * XB, XB), XB)], ob.at[lax.rem(k, 2)], xsem.at[lax.rem(k, 2)])

    for src, dst in ((x_h, xt), (dy_h, dyt)):
        xload(0, src).start()

        def tr(k, _, src=src, dst=dst):
            @pl.when(k + 1 < nx)
            def _():
                xload(k + 1, src).start()
            xload(k, src).wait()
            dst[:, pl.ds(pl.multiple_of(k * XB, XB), XB)] = ob[lax.rem(k, 2)].T
            return 0
        lax.fori_loop(0, nx, tr, 0)

    def zero(k, _):
        acc[:, pl.ds(pl.multiple_of(k * 256, 256), 256)] = jnp.zeros((D, 256), F32)
        return 0
    lax.fori_loop(0, N // 256, zero, 0)

    def trans(src, dst):
        for k in range(D // 128):
            ck = pl.ds(k * 128, 128)
            wn[dst, ck, 0:FT] = wb[src, 0:FT, ck].T
            wn[dst, ck, FT:2 * FT] = wb[src, FT:2 * FT, ck].T

    def stage1(it, gb):
        j = it // C
        ws = lax.rem(j, 3)
        cols = pl.ds(pl.multiple_of(lax.rem(it, C) * T, T), T)
        ab = jnp.dot(wb[ws, 0:2 * FT, :], xt[:, cols], preferred_element_type=F32)
        dh = jnp.dot(wb[ws, 2 * FT:3 * FT, :], dyt[:, cols], preferred_element_type=F32)
        a = ab[:FT]
        b = ab[FT:]
        sg = jax.nn.sigmoid(a)
        act = a * sg
        gb[2 * FT:3 * FT, :] = (act * b).astype(BF16)
        gb[FT:2 * FT, :] = (dh * act).astype(BF16)
        gb[0:FT, :] = (dh * b * sg * (1.0 + a * (1.0 - sg))).astype(BF16)

    def stage2(it, gb):
        ck = lax.rem(it, C)
        ns = lax.rem(it // C, 2)
        cols = pl.ds(pl.multiple_of(ck * T, T), T)
        acc[:, cols] += jnp.dot(wn[ns], gb[0:2 * FT, :], preferred_element_type=F32)
        d1 = lax.dot_general(xt[:, cols], gb[0:2 * FT, :], NT, preferred_element_type=F32)
        d2 = lax.dot_general(dyt[:, cols], gb[2 * FT:3 * FT, :], NT, preferred_element_type=F32)
        first = ck == 0
        dwb[ns, 0] = jnp.where(first, 0.0, dwb[ns, 0]) + d1[:, :FT]
        dwb[ns, 1] = jnp.where(first, 0.0, dwb[ns, 1]) + d1[:, FT:]
        dwb[ns, 2] = jnp.where(first, 0.0, dwb[ns, 2]) + d2

    def dcopy(j):
        sl = lax.rem(j, 2)
        return pltpu.make_async_copy(dwb.at[sl], dw_h.at[:, :, pl.ds(pl.multiple_of(tile(j) * FT, 128), FT)], dsem.at[sl])

    def ocopy(k):
        return pltpu.make_async_copy(ob.at[lax.rem(k, 2)], dx_h.at[pl.ds(pl.multiple_of(k * XB, XB), XB)], osem.at[lax.rem(k, 2)])

    def unit(u):
        return u // 14, lax.rem(u, 14) // 2, lax.rem(u, 2)

    def gload(u, cc, buf, sem):
        k, i, h = unit(u)
        sl = lax.rem(u, 2)
        out = []
        for q in range(2):
            col = q * (FF // 2) + cc * 1152 + h * UC
            out.append(pltpu.make_async_copy(g_h.at[k, pl.ds(pl.multiple_of(i * UR, UR), UR), pl.ds(pl.multiple_of(col, 128), UC)], buf.at[sl, q], sem.at[sl, q]))
        return out

    def load_a(u):
        return gload(u, 1 - c, ga, gas)

    def load_b(u):
        return gload(u, c, gb_in, gbs) + [pltpu.make_async_copy(ra_h.at[u], ra.at[lax.rem(u, 2)], ras.at[lax.rem(u, 2)])]

    def send_a(u):
        return remote(sa.at[lax.rem(u, 3)], ra_h.at[u], sas.at[u], sar.at[u], core)

    def send_x(u):
        return remote(pb.at[lax.rem(u, PS), 1 - r], rx_h.at[u], sxs.at[u], sxr.at[u], xnb)

    def send_y(u):
        return remote(qb.at[lax.rem(u, QS)], ry_h.at[u], sys_.at[u], syr.at[u], ynb)

    def load_c(u):
        return pltpu.make_async_copy(rx_h.at[u], rx.at[lax.rem(u, 2)], rxs.at[lax.rem(u, 2)])

    def load_d(u):
        return pltpu.make_async_copy(ry_h.at[u], ry.at[lax.rem(u, 2)], rys.at[lax.rem(u, 2)])

    def out_d(bk):
        sl = lax.rem(bk, 2)
        return pltpu.make_async_copy(tb.at[sl, pl.ds(pl.multiple_of(64 * c, 64), SH)], dn_h.at[bk // 7, :, pl.ds(pl.multiple_of(lax.rem(bk, 7) * UR, UR), UR)], tbs.at[sl])

    def on(u):
        return (u >= 0) & (u < UN)

    def background(it):
        for w in range(3):
            @pl.when(it == 8 + 5 * w)
            def _(w=w):
                ag(1, w).wait_recv()
                ag(2, w).start()
                ag(3, w).start()

            @pl.when(it == 15 + 5 * w)
            def _(w=w):
                ag(2, w).wait_recv()
                ag(4, w).start()
        ua, ub, uc, ud = it - A0, it - B0, it - C0, it - D0

        @pl.when(on(ua - 1))
        def _():
            send_a(ua - 1).start()

        @pl.when(on(ub - 1))
        def _():
            send_x(ub - 1).start()

        @pl.when(on(uc - 1))
        def _():
            send_y(uc - 1).start()

        @pl.when(on(ua + 1))
        def _():
            for cp in load_a(ua + 1):
                cp.start()

        @pl.when(on(ub + 1))
        def _():
            send_a(ub + 1).wait_recv()
            for cp in load_b(ub + 1):
                cp.start()

        @pl.when(on(uc + 1))
        def _():
            send_x(uc + 1).wait_recv()
            load_c(uc + 1).start()

        @pl.when(on(ud + 1))
        def _():
            send_y(ud + 1).wait_recv()
            load_d(ud + 1).start()

        @pl.when(on(ua))
        def _():
            @pl.when(ua >= 3)
            def _():
                send_a(ua - 3).wait_send()
            for cp in load_a(ua):
                cp.wait()
            sa[lax.rem(ua, 3)] = ga[lax.rem(ua, 2)].astype(BF16)

        @pl.when(on(ub))
        def _():
            @pl.when(ub >= PS)
            def _():
                send_x(ub - PS).wait_send()
            for cp in load_b(ub):
                cp.wait()
            sl = lax.rem(ub, 2)
            pb[lax.rem(ub, PS)] = (gb_in[sl].astype(BF16).astype(F32) + ra[sl].astype(F32)).astype(BF16)

        @pl.when(on(uc))
        def _():
            @pl.when(uc >= QS)
            def _():
                send_y(uc - QS).wait_send()
            load_c(uc).wait()
            qb[lax.rem(uc, QS)] = (pb[lax.rem(uc, PS), r].astype(F32) + rx[lax.rem(uc, 2)].astype(F32)).astype(BF16)

        @pl.when(on(ud))
        def _():
            bk = ud // 2
            h = lax.rem(ud, 2)

            @pl.when((h == 0) & (bk >= 2))
            def _():
                out_d(bk - 2).wait()
            load_d(ud).wait()
            tot = qb[lax.rem(ud, QS)].astype(F32) + ry[lax.rem(ud, 2)].astype(F32)
            tb[lax.rem(bk, 2), pl.ds(pl.multiple_of(h * UC, 128), UC), :] = tot.T

            @pl.when(h == 1)
            def _():
                out_d(bk).start()

    for cp in wcopy(0, 0, True):
        cp.wait()
    trans(0, 0)
    stage1(0, gba)

    def body(it, src, dst):
        j = it // C
        ck = lax.rem(it, C)
        jp = (it - 1) // C
        cp_ = lax.rem(it - 1, C)

        @pl.when((ck == 1) & (j + 1 < NF) & (j > 0))
        def _():
            @pl.when(j + 1 < 4)
            def _():
                for cp in wcopy(j + 1, lax.rem(j + 1, 3), True):
                    cp.start()

            @pl.when(j + 1 >= 4)
            def _():
                @pl.when(j + 1 == 4)
                def _():
                    for w in range(3):
                        for e in range(2):
                            edge(w, e).wait()
                        ag(0, w).wait_recv()

                @pl.when(j + 1 == 9)
                def _():
                    for w in range(3):
                        ag(3, w).wait_recv()
                        ag(4, w).wait_recv()
                for cp in wcopy(j + 1, lax.rem(j + 1, 3), False):
                    cp.start()

        background(it)

        @pl.when((ck == 0) & (j < NF))
        def _():
            for cp in wcopy(j, lax.rem(j, 3), False):
                cp.wait()
            trans(lax.rem(j, 3), lax.rem(j, 2))

        @pl.when((cp_ == 0) & (jp >= 2))
        def _():
            dcopy(jp - 2).wait()
        stage1(it, dst)
        stage2(it - 1, src)

        @pl.when(cp_ == C - 1)
        def _():
            dcopy(jp).start()

        @pl.when(jp == NF - 1)
        def _():
            for q in range(T // XB):
                k = cp_ * (T // XB) + q

                @pl.when(k >= 2)
                def _():
                    ocopy(k - 2).wait()
                ob[q % 2] = acc[:, pl.ds(pl.multiple_of(k * XB, XB), XB)].astype(BF16).T
                ocopy(k).start()

    def pair(i, _):
        body(2 * i + 1, gba, gbb)
        body(2 * i + 2, gbb, gba)
        return 0
    lax.fori_loop(0, NF * C // 2, pair, 0)

    dcopy(NF - 2).wait()
    dcopy(NF - 1).wait()
    ocopy(N // XB - 2).wait()
    ocopy(N // XB - 1).wait()
    out_d(19).wait()
    out_d(20).wait()
    for w in range(3):
        for kind in range(5):
            ag(kind, w).wait_send()
    for u in range(UN - 3, UN):
        send_a(u).wait_send()
    for u in range(UN - PS, UN):
        send_x(u).wait_send()
    for u in range(UN - QS, UN):
        send_y(u).wait_send()


def solution(mesh):
    def local_step(x_dev, dy_dev, gate_shard, up_shard, down_shard, g_dev):
        any_spec = pl.BlockSpec(memory_space=pl.ANY)
        sds = jax.ShapeDtypeStruct
        dma = pltpu.SemaphoreType.DMA
        vm = pltpu.VMEM
        outs = pl.pallas_call(
            step_kernel,
            in_specs=[any_spec] * 6,
            out_specs=[any_spec] * 9,
            out_shape=[sds((3, D, FF), F32), sds((N, D), BF16), sds((3, SH, D), F32),
                       sds((FF, D), BF16), sds((FF, D), BF16), sds((FF, D), BF16),
                       sds((UN, 2, UR, UC), BF16), sds((UN, UR, UC), BF16), sds((UN, UR, UC), BF16)],
            scratch_shapes=[
                vm((D, N), BF16), vm((D, N), BF16), vm((D, N), F32),
                vm((3, 3 * FT, D), BF16), vm((2, D, 2 * FT), BF16), vm((2, 3, D, FT), F32),
                vm((3 * FT, T), BF16), vm((3 * FT, T), BF16), vm((2, XB, D), BF16),
                vm((2, 2, UR, UC), F32), vm((2, 2, UR, UC), F32), vm((3, 2, UR, UC), BF16),
                vm((2, 2, UR, UC), BF16), vm((PS, 2, UR, UC), BF16), vm((2, UR, UC), BF16),
                vm((QS, UR, UC), BF16), vm((2, UR, UC), BF16), vm((2, 2 * UC, UR), F32),
                dma((3, 3)), dma((2,)), dma((2,)), dma((2,)), dma((1,)), dma((3, 2)), dma((5, 3)), dma((5, 3)),
                dma((2, 2)), dma((2, 2)), dma((2,)), dma((2,)), dma((2,)), dma((2,)),
                dma((UN,)), dma((UN,)), dma((UN,)), dma((UN,)), dma((UN,)), dma((UN,)),
            ],
            compiler_params=pltpu.CompilerParams(collective_id=0, has_side_effects=True, vmem_limit_bytes=65470 * 1024),
        )(x_dev.reshape(N, D), dy_dev.reshape(N, D), gate_shard.T, up_shard.T, down_shard, g_dev[0])
        dw, dx, dn = outs[:3]
        return dx.reshape(2, N // 2, D), dn.transpose(0, 2, 1), dw[None]

    in_specs = (P(None, TOK_AXES, None), P(None, TOK_AXES, None), P(None, GROUP_AXES), P(None, GROUP_AXES), P(GROUP_AXES, None), P(TOK_AXES, None, None, None))
    out_specs = (P(None, TOK_AXES, None), P(None, None, GROUP_AXES), P(TOK_AXES, None, None, None))
    return jax.shard_map(local_step, mesh=mesh, in_specs=in_specs, out_specs=out_specs, check_vma=False)
```

```python
import functools

import jax
import jax.numpy as jnp
from jax import lax
from jax.experimental import pallas as pl
from jax.experimental.pallas import tpu as pltpu
from jax.sharding import PartitionSpec as P

TOK_AXES = ("dp", "row", "fsdp")
GROUP_AXES = ("row", "fsdp")

D = 896
FF = 4864
N = 4096
SH = FF // 4
FT = 256
T = 1024
NF = FF // FT
TW = 512
NW = FF // TW
TL = FF - NW * TW
C = N // T
TP = 512
XS = 6
XB = 256
UN = 21
UR, UC = 128, 1280
A0, B0, C0, D0 = 6, 8, 11, 14
PS, QS = C0 - B0 + 1, D0 - C0 + 1
NT = (((1,), (1,)), ((), ()))
F32, BF16 = jnp.float32, jnp.bfloat16
MESH = pl.DeviceIdType.MESH


def step_kernel(x_h, dy_h, w1_h, w3_h, w2_h, g_h,
                dw_h, dx_h, dn_h, wg1, wg3, wg2, ra_h, rx_h, ry_h, db_h, hh_h, xt_h, dyt_h,
                xt, dyt, acc, wb, wn, dwb, gba, gbb, raw2, ob,
                ga, gb_in, sa, ra, pb, rx, qb, ry, tb,
                wsem, dsem, xsem, osem, lsem, agl, ags, agr,
                gas, gbs, ras, rxs, rys, tbs, gos, xos, sas, sar, sxs, sxr, sys_, syr):
    d = lax.axis_index("dp")
    r = lax.axis_index("row")
    c = lax.axis_index("fsdp")
    core = (d, r, 1 - c)
    xnb = (d, 1 - r, c)
    ynb = (1 - d, r, c)
    s = 2 * r + c
    so = 2 * (1 - r) + c

    bar = pltpu.get_barrier_semaphore()
    for dev in (core, xnb, ynb):
        pl.semaphore_signal(bar, inc=1, device_id=dev, device_id_type=MESH)
    pl.semaphore_wait(bar, 3)

    own = (w1_h, w3_h, w2_h)
    full = (wg1, wg3, wg2)

    def rows(start, size):
        return pl.ds(pl.multiple_of(start, 32), size)

    def remote(src, dst, ssem, rsem, dev):
        return pltpu.make_async_remote_copy(src_ref=src, dst_ref=dst, send_sem=ssem, recv_sem=rsem, device_id=dev, device_id_type=MESH)

    H = SH // 2

    def ag(kind, w):
        if kind == 0:
            return remote(own[w], full[w].at[rows(s * SH, SH)], ags.at[kind, w], agr.at[kind, w], core)
        if kind == 1:
            return remote(own[w].at[rows(d * H, H)], full[w].at[rows(s * SH + d * H, H)], ags.at[kind, w], agr.at[kind, w], xnb)
        got = full[w].at[rows(so * SH + d * H, H)]
        if kind == 2:
            return remote(got, got, ags.at[kind, w], agr.at[kind, w], ynb)
        if kind == 3:
            return remote(got, got, ags.at[kind, w], agr.at[kind, w], core)
        got = full[w].at[rows(so * SH + (1 - d) * H, H)]
        return remote(got, got, ags.at[kind, w], agr.at[kind, w], core)

    for w in range(3):
        ag(1, w).start()
    for w in range(3):
        ag(0, w).start()

    def edge(w, e):
        off = e * (SH - 192)
        return pltpu.make_async_copy(own[w].at[rows(off, 192)], full[w].at[rows(s * SH + off, 192)], agl.at[w, e])

    for w in range(3):
        for e in range(2):
            edge(w, e).start()

    def tile(j):
        one = jnp.where(j < 4, 5 + j, jnp.where(j < 9, 8 - j, jnp.where(j < 13, 6 + j, 27 - j)))
        zero = j
        t = jnp.where(r == c, zero, one)
        return jnp.where(r == 1, NF - 1 - t, t)

    def wcopy(j, slot, mine):
        t = tile(j)
        out = []
        for w in range(3):
            if mine:
                src = own[w].at[rows(t * FT - s * SH, FT)]
            else:
                src = full[w].at[rows(t * FT, FT)]
            out.append(pltpu.make_async_copy(src, wb.at[slot, pl.ds(w * FT, FT)], wsem.at[slot, w]))
        return out

    for cp in wcopy(0, 0, True):
        cp.start()
    for cp in wcopy(1, 1, True):
        cp.start()

    nx = N // XB

    def xload(k, act):
        sl = lax.rem(k, XS)
        rs = pl.ds(pl.multiple_of(lax.rem(k, nx) * XB, XB), XB)

        @pl.when(k < nx)
        def _():
            getattr(pltpu.make_async_copy(x_h.at[rs], ob.at[sl], xsem.at[sl]), act)()

        @pl.when(k >= nx)
        def _():
            getattr(pltpu.make_async_copy(dy_h.at[rs], ob.at[sl], xsem.at[sl]), act)()

    for k in range(XS - 1):
        xload(k, "start")

    def tr(k, _, dst=None):
        @pl.when(k + XS - 1 < 2 * nx)
        def _():
            xload(k + XS - 1, "start")
        xload(k, "wait")
        dst[:, pl.ds(pl.multiple_of(lax.rem(k, nx) * XB, XB), XB)] = ob[lax.rem(k, XS)].T
        return 0
    lax.fori_loop(0, nx, functools.partial(tr, dst=xt), 0)
    lax.fori_loop(nx, 2 * nx, functools.partial(tr, dst=dyt), 0)

    keep = (pltpu.make_async_copy(xt, xt_h, xos.at[0]), pltpu.make_async_copy(dyt, dyt_h, xos.at[1]))
    for cp in keep:
        cp.start()

    def zero(k, _):
        acc[:, pl.ds(pl.multiple_of(k * 256, 256), 256)] = jnp.zeros((D, 256), F32)
        return 0
    lax.fori_loop(0, N // 256, zero, 0)

    def trans(src, dst, k):
        ck = pl.ds(pl.multiple_of(k * 128, 128), 128)
        wn[dst, ck, 0:FT] = wb[src, 0:FT, ck].T
        wn[dst, ck, FT:2 * FT] = wb[src, FT:2 * FT, ck].T

    def products(it, raw):
        ck = lax.rem(it, C)
        ws = lax.rem(it // C, 3)

        def piece(half, p):
            to = pl.ds(p * TP, TP)
            cols = pl.ds(pl.multiple_of(ck * T + p * TP, TP), TP)
            if half == 0:
                raw[0:2 * FT, to] = jnp.dot(wb[ws, 0:2 * FT, :], xt[:, cols], preferred_element_type=F32)
            else:
                raw[2 * FT:3 * FT, to] = jnp.dot(wb[ws, 2 * FT:3 * FT, :], dyt[:, cols], preferred_element_type=F32)
        return [functools.partial(piece, half, p) for half in range(2) for p in range(T // TP)]

    def gates(raw, gb):
        def piece(i, p):
            to = pl.ds(p * 512, 512)
            a = raw[pl.ds(i * 16, 16), to]
            b = raw[pl.ds(FT + i * 16, 16), to]
            dh = raw[pl.ds(2 * FT + i * 16, 16), to]
            sg = jax.nn.sigmoid(a)
            act = a * sg
            gb[pl.ds(2 * FT + i * 16, 16), to] = (act * b).astype(BF16)
            gb[pl.ds(FT + i * 16, 16), to] = (dh * act).astype(BF16)
            gb[pl.ds(i * 16, 16), to] = (dh * b * sg * (1.0 + a * (1.0 - sg))).astype(BF16)
        return [functools.partial(piece, i, p) for p in range(T // 512) for i in range(FT // 16)]

    def add_dx(it, gb):
        ck = lax.rem(it, C)
        ns = lax.rem(it // C, 3)

        def piece(p):
            cols = pl.ds(pl.multiple_of(ck * T + p * TP, TP), TP)
            acc[:, cols] += jnp.dot(wn[ns], gb[0:2 * FT, p * TP:(p + 1) * TP], preferred_element_type=F32)
        return [functools.partial(piece, p) for p in range(T // TP)]

    def add_dw(it, gb):
        ck = lax.rem(it, C)
        ns = lax.rem(it // C, 2)
        cols = pl.ds(pl.multiple_of(ck * T, T), T)

        def piece(p):
            mr = pl.ds(p * (D // 2), D // 2)
            d0 = lax.dot_general(xt[mr, cols], gb[0:FT, :], NT, preferred_element_type=F32)
            dwb[ns, mr] = jnp.where(ck == 0, 0.0, dwb[ns, mr]) + d0
        return [functools.partial(piece, p) for p in range(2)]

    def dcopy(j):
        sl = lax.rem(j, 2)
        return pltpu.make_async_copy(dwb.at[sl], dw_h.at[:, pl.ds(pl.multiple_of(tile(j) * FT, 128), FT)], dsem.at[sl])

    def gcopy(it, gb, sl):
        rs = rows(tile(it // C) * FT, FT)
        cs = pl.ds(pl.multiple_of(lax.rem(it, C) * T, T), T)
        return [pltpu.make_async_copy(gb.at[pl.ds(FT, FT)], db_h.at[rs, cs], gos.at[sl, 0]),
                pltpu.make_async_copy(gb.at[pl.ds(2 * FT, FT)], hh_h.at[rs, cs], gos.at[sl, 1])]

    def ocopy(k):
        return pltpu.make_async_copy(ob.at[lax.rem(k, 2)], dx_h.at[pl.ds(pl.multiple_of(k * XB, XB), XB)], osem.at[lax.rem(k, 2)])

    def unit(u):
        return u // 7, lax.rem(u, 7)

    def gload(u, cc, buf, sem):
        k, i = unit(u)
        out = []
        for q in range(2):
            col = q * (FF // 2) + cc * 1152
            out.append(pltpu.make_async_copy(g_h.at[k, pl.ds(pl.multiple_of(i * UR, UR), UR), pl.ds(pl.multiple_of(col, 128), UC)], buf.at[q], sem.at[q]))
        return out

    def load_a(u):
        return gload(u, 1 - c, ga, gas)

    def load_b(u):
        return gload(u, c, gb_in, gbs) + [pltpu.make_async_copy(ra_h.at[u], ra, ras.at[0])]

    def send_a(u):
        return remote(sa.at[lax.rem(u, 2)], ra_h.at[u], sas.at[u], sar.at[u], core)

    def send_x(u):
        return remote(pb.at[lax.rem(u, PS), 1 - r], rx_h.at[u], sxs.at[u], sxr.at[u], xnb)

    def send_y(u):
        return remote(qb.at[lax.rem(u, QS)], ry_h.at[u], sys_.at[u], syr.at[u], ynb)

    def load_c(u):
        return pltpu.make_async_copy(rx_h.at[u], rx, rxs.at[0])

    def load_d(u):
        return pltpu.make_async_copy(ry_h.at[u], ry, rys.at[0])

    def out_d(u):
        sl = lax.rem(u, 2)
        return pltpu.make_async_copy(tb.at[sl, pl.ds(pl.multiple_of(64 * c, 64), SH)], dn_h.at[u // 7, :, pl.ds(pl.multiple_of(lax.rem(u, 7) * UR, UR), UR)], tbs.at[sl])

    def on(u):
        return (u >= 0) & (u < UN)

    def forward(it):
        for w in range(3):
            @pl.when(it == 6 + 6 * w)
            def _(w=w):
                ag(1, w).wait_recv()
                ag(2, w).start()
                ag(3, w).start()

            @pl.when(it == (14, 20, 28)[w])
            def _(w=w):
                ag(2, w).wait_recv()
                ag(4, w).start()

    def first_half(i):
        ua, ub, uc, ud = i - A0, i - B0, i - C0, i - D0

        @pl.when(on(uc - 1))
        def _():
            send_y(uc - 1).start()

        @pl.when(on(uc))
        def _():
            send_x(uc).wait_recv()
            load_c(uc).start()

        @pl.when(on(ud))
        def _():
            send_y(ud).wait_recv()
            load_d(ud).start()

        @pl.when(on(ua))
        def _():
            @pl.when(ua >= 2)
            def _():
                send_a(ua - 2).wait_send()
            for cp in load_a(ua):
                cp.wait()

        @pl.when(on(ub))
        def _():
            @pl.when(ub >= PS)
            def _():
                send_x(ub - PS).wait_send()
            for cp in load_b(ub):
                cp.wait()

    def second_half(i):
        ua, ub, uc, ud = i - A0, i - B0, i - C0, i - D0

        @pl.when(on(ua))
        def _():
            send_a(ua).start()

        @pl.when(on(ub))
        def _():
            send_x(ub).start()

        @pl.when(on(ua + 1))
        def _():
            for cp in load_a(ua + 1):
                cp.start()

        @pl.when(on(ub + 1))
        def _():
            send_a(ub + 1).wait_recv()
            for cp in load_b(ub + 1):
                cp.start()

        @pl.when(on(uc))
        def _():
            @pl.when(uc >= QS)
            def _():
                send_y(uc - QS).wait_send()
            load_c(uc).wait()

        @pl.when(on(ud))
        def _():
            @pl.when(ud >= 2)
            def _():
                out_d(ud - 2).wait()
            load_d(ud).wait()

    def mod(u, n):
        return lax.rem(u + 40 * n, n)

    def spot(u, n):
        return jnp.where(on(u), mod(u, n), n)

    def arith_ab(i):
        da, db = spot(i - A0, 2), spot(i - B0, PS)

        def cast(q, n):
            rs = pl.ds(n * 16, 16)
            sa[da, q, rs] = ga[q, rs].astype(BF16)

        def core_sum(q, n):
            rs = pl.ds(n * 16, 16)
            pb[db, q, rs] = (gb_in[q, rs].astype(BF16).astype(F32) + ra[q, rs].astype(F32)).astype(BF16)
        return [functools.partial(f, q, n) for q in range(2) for n in range(UR // 16) for f in (cast, core_sum)]

    def arith_cd(i):
        uc, ud = i - C0, i - D0
        dc, dd = spot(uc, QS), spot(ud, 2)

        def row_sum(n):
            rs = pl.ds(n * 16, 16)
            qb[dc, rs] = (pb[mod(uc, PS), r, rs].astype(F32) + rx[rs].astype(F32)).astype(BF16)

        def dp_sum(n):
            cs = pl.ds(n * 128, 128)
            tot = qb[mod(ud, QS), :, cs].astype(F32) + ry[:, cs].astype(F32)
            tb[dd, pl.ds(n * 128, 128), :] = tot.T
        return [functools.partial(dp_sum, n) for n in range(UC // 128)] + [functools.partial(row_sum, n) for n in range(UR // 16)]

    def flush(i):
        @pl.when(on(i - D0))
        def _():
            out_d(i - D0).start()

    for cp in wcopy(0, 0, True):
        cp.wait()
    for k in range(D // 128):
        trans(0, 0, k)
    for cp in wcopy(1, 1, True):
        cp.wait()
    for k in range(2):
        trans(1, 1, k)
    gbs2 = (gba, gbb)

    def body(it, par, step=None):
        j = it // C
        ck = lax.rem(it, C)
        jp = (it - 1) // C
        cp_ = lax.rem(it - 1, C)
        jn = j + 2

        @pl.when((ck == 1) & (jn < NF))
        def _():
            @pl.when(jn < 4)
            def _():
                for cp in wcopy(jn, lax.rem(jn, 3), True):
                    cp.start()

            @pl.when(jn >= 4)
            def _():
                @pl.when(jn == 4)
                def _():
                    for w in range(3):
                        for e in range(2):
                            edge(w, e).wait()
                        ag(0, w).wait_recv()

                @pl.when(jn == 9)
                def _():
                    for w in range(3):
                        ag(3, w).wait_recv()
                        ag(4, w).wait_recv()
                for cp in wcopy(jn, lax.rem(jn, 3), False):
                    cp.start()

        @pl.when((ck == 0) & (j + 1 < NF))
        def _():
            for cp in wcopy(j + 1, lax.rem(j + 1, 3), False):
                cp.wait()

        side = []
        if step is not None:
            if par == 0:
                forward(it)
                first_half(step)
                side = arith_ab(step)
            else:
                second_half(step)
                side = arith_cd(step)
        for cp in gcopy(it - 1, gbs2[1 - par], 1 - par):
            cp.start()

        @pl.when(it >= 2)
        def _():
            for cp in gcopy(it - 2, gbs2[par], par):
                cp.wait()

        @pl.when((cp_ == 0) & (jp >= 2))
        def _():
            dcopy(jp - 2).wait()
        prod, gate = products(it, raw2), gates(raw2, gbs2[par])
        grad = add_dx(it - 1, gbs2[1 - par]) + add_dw(it - 1, gbs2[1 - par])
        side += [functools.partial(trans, lax.rem(j + 1, 3), lax.rem(j + 1, 3), jnp.minimum(2 * ck + q, D // 128 - 1)) for q in range(2)]
        ng, nd = len(gate) // 2, len(side) // 2
        run(prod[0], prod[2], prod[1], *gate[:ng], prod[3], *side[:nd], *grad[:1], *gate[ng:], *grad[1:2], *side[nd:], *grad[2:])
        if step is not None and par == 1:
            flush(step)
        grads_out(jp, cp_)

    def run(*fs):
        for f in fs:
            f()

    def grads_out(jp, cp_):
        @pl.when(cp_ == C - 1)
        def _():
            dcopy(jp).start()

        @pl.when(jp == NF - 1)
        def _():
            for q in range(T // XB):
                k = cp_ * (T // XB) + q

                @pl.when(k >= 2)
                def _():
                    ocopy(k - 2).wait()
                ob[q % 2] = acc[:, pl.ds(pl.multiple_of(k * XB, XB), XB)].astype(BF16).T
                ocopy(k).start()

    run(*products(0, raw2), *gates(raw2, gba))
    body(1, 1)

    def pair(i, _):
        body(2 * i + 2, 0, i)
        body(2 * i + 3, 1, i)
        return 0
    lax.fori_loop(0, NF * C // 2 - 1, pair, 0)
    last = NF * C - 1
    for cp in gcopy(last, gbb, 1):
        cp.start()
    for cp in gcopy(last - 1, gba, 0):
        cp.wait()
    run(*add_dx(last, gbb), *add_dw(last, gbb))
    grads_out(NF - 1, C - 1)

    dcopy(NF - 2).wait()
    dcopy(NF - 1).wait()
    for cp in gcopy(NF * C - 1, gbb, 1):
        cp.wait()
    for cp in keep:
        cp.wait()
    ocopy(N // XB - 2).wait()
    ocopy(N // XB - 1).wait()
    out_d(19).wait()
    out_d(20).wait()
    for w in range(3):
        for kind in range(5):
            ag(kind, w).wait_send()
    for u in range(UN - 2, UN):
        send_a(u).wait_send()
    for u in range(UN - PS, UN):
        send_x(u).wait_send()
    for u in range(UN - QS, UN):
        send_y(u).wait_send()


def tail_kernel(xt_h, dyt_h, db_h, hh_h, d0_h, dxi_h, dni_h, dw_h, dx_h, dn_h,
                xt, dyt, db, hh, ow, bx, bn, xsem, gsem, osem, dsem, bsem, csem):
    def part(j, width):
        return pl.ds(pl.multiple_of(j * TW, TW), width)

    def loads(j, width):
        sl = lax.rem(j, 2)
        to = pl.ds(0, width)
        return [pltpu.make_async_copy(db_h.at[part(j, width)], db.at[sl, to], gsem.at[sl, 0]),
                pltpu.make_async_copy(hh_h.at[part(j, width)], hh.at[sl, to], gsem.at[sl, 1])]

    def slab0(j, width):
        sl = lax.rem(j, 2)
        return pltpu.make_async_copy(d0_h.at[:, part(j, width)], ow.at[sl, 0, :, pl.ds(0, width)], dsem.at[sl])

    def out(j, width):
        sl = lax.rem(j, 2)
        return pltpu.make_async_copy(ow.at[sl, :, :, pl.ds(0, width)], dw_h.at[:, :, part(j, width)], osem.at[sl])

    def carry(j, put):
        sl = lax.rem(j, 2)
        rx = pl.ds(pl.multiple_of(j * (N // 8), 128), N // 8)
        rn = pl.ds(pl.multiple_of(j * (SH // 8), 8), SH // 8)
        if put:
            return (pltpu.make_async_copy(bx.at[sl], dx_h.at[rx], csem.at[sl, 0]),
                    pltpu.make_async_copy(bn.at[sl], dn_h.at[:, rn], csem.at[sl, 1]))
        return (pltpu.make_async_copy(dxi_h.at[rx], bx.at[sl], bsem.at[sl, 0]),
                pltpu.make_async_copy(dni_h.at[:, rn], bn.at[sl], bsem.at[sl, 1]))

    ldx = pltpu.make_async_copy(xt_h, xt, xsem.at[0])
    ldy = pltpu.make_async_copy(dyt_h, dyt, xsem.at[1])
    first = loads(0, TW)
    first[0].start()
    ldx.start()
    first[1].start()
    ldy.start()
    slab0(0, TW).start()
    for cp in carry(0, False):
        cp.start()

    def step(j, _):
        sl = lax.rem(j, 2)

        @pl.when(j == 0)
        def _():
            ldx.wait()
            ldy.wait()

        @pl.when((j >= 1) & (j <= 8))
        def _():
            for cp in carry(j - 1, False):
                cp.wait()
            for cp in carry(j - 1, True):
                cp.start()

        @pl.when(j < NW - 1)
        def _():
            for cp in loads(j + 1, TW):
                cp.start()

        @pl.when(j == NW - 1)
        def _():
            for cp in loads(j + 1, TL):
                cp.start()
        for cp in loads(j, TW):
            cp.wait()
        ow[sl, 1] = lax.dot_general(xt[...], db[sl], NT, preferred_element_type=F32)

        @pl.when(j >= 1)
        def _():
            out(j - 1, TW).wait()
            for cp in carry(j - 1, True):
                cp.wait()

        @pl.when(j < NW - 1)
        def _():
            slab0(j + 1, TW).start()

        @pl.when(j == NW - 1)
        def _():
            slab0(j + 1, TL).start()

        @pl.when(j + 1 < 8)
        def _():
            for cp in carry(j + 1, False):
                cp.start()
        ow[sl, 2] = lax.dot_general(dyt[...], hh[sl], NT, preferred_element_type=F32)
        slab0(j, TW).wait()
        out(j, TW).start()
        return 0
    lax.fori_loop(0, NW, step, 0)

    for cp in loads(NW, TL):
        cp.wait()
    sl = NW % 2
    for p in range(2):
        mr = pl.ds(p * (D // 2), D // 2)
        ow[sl, 1, mr, 0:TL] = lax.dot_general(xt[mr], db[sl, 0:TL], NT, preferred_element_type=F32)
        ow[sl, 2, mr, 0:TL] = lax.dot_general(dyt[mr], hh[sl, 0:TL], NT, preferred_element_type=F32)
    slab0(NW, TL).wait()
    out(NW, TL).start()
    out(NW - 1, TW).wait()
    out(NW, TL).wait()


def solution(mesh):
    def local_step(x_dev, dy_dev, gate_shard, up_shard, down_shard, g_dev):
        any_spec = pl.BlockSpec(memory_space=pl.ANY)
        sds = jax.ShapeDtypeStruct
        dma = pltpu.SemaphoreType.DMA
        vm = pltpu.VMEM
        outs = pl.pallas_call(
            step_kernel,
            in_specs=[any_spec] * 6,
            out_specs=[any_spec] * 13,
            out_shape=[sds((D, FF), F32), sds((N, D), BF16), sds((3, SH, D), F32),
                       sds((FF, D), BF16), sds((FF, D), BF16), sds((FF, D), BF16),
                       sds((UN, 2, UR, UC), BF16), sds((UN, UR, UC), BF16), sds((UN, UR, UC), BF16),
                       sds((FF, N), BF16), sds((FF, N), BF16), sds((D, N), BF16), sds((D, N), BF16)],
            scratch_shapes=[
                vm((D, N), BF16), vm((D, N), BF16), vm((D, N), F32),
                vm((3, 3 * FT, D), BF16), vm((3, D, 2 * FT), BF16), vm((2, D, FT), F32),
                vm((3 * FT, T), BF16), vm((3 * FT, T), BF16), vm((3 * FT, T), F32), vm((XS, XB, D), BF16),
                vm((2, UR, UC), F32), vm((2, UR, UC), F32), vm((3, 2, UR, UC), BF16),
                vm((2, UR, UC), BF16), vm((PS + 1, 2, UR, UC), BF16), vm((UR, UC), BF16),
                vm((QS + 1, UR, UC), BF16), vm((UR, UC), BF16), vm((3, UC, UR), F32),
                dma((3, 3)), dma((2,)), dma((XS,)), dma((2,)), dma((1,)), dma((3, 2)), dma((5, 3)), dma((5, 3)),
                dma((2,)), dma((2,)), dma((1,)), dma((1,)), dma((1,)), dma((2,)), dma((2, 2)), dma((2,)),
                dma((UN,)), dma((UN,)), dma((UN,)), dma((UN,)), dma((UN,)), dma((UN,)),
            ],
            compiler_params=pltpu.CompilerParams(collective_id=0, has_side_effects=True, vmem_limit_bytes=65470 * 1024),
        )(x_dev.reshape(N, D), dy_dev.reshape(N, D), gate_shard.T, up_shard.T, down_shard, g_dev[0])
        dw, dx, dn = pl.pallas_call(
            tail_kernel,
            in_specs=[any_spec] * 7,
            out_specs=[any_spec] * 3,
            out_shape=[sds((3, D, FF), F32), sds((N, D), BF16), sds((3, SH, D), F32)],
            scratch_shapes=[
                vm((D, N), BF16), vm((D, N), BF16), vm((2, TW, N), BF16), vm((2, TW, N), BF16), vm((2, 3, D, TW), F32),
                vm((2, N // 8, D), BF16), vm((2, 3, SH // 8, D), F32),
                dma((2,)), dma((2, 2)), dma((2,)), dma((2,)), dma((2, 2)), dma((2, 2)),
            ],
            compiler_params=pltpu.CompilerParams(vmem_limit_bytes=60 * 1024 * 1024),
        )(outs[11], outs[12], outs[9], outs[10], outs[0], outs[1], outs[2])
        return dx.reshape(2, N // 2, D), dn.transpose(0, 2, 1), dw[None]

    in_specs = (P(None, TOK_AXES, None), P(None, TOK_AXES, None), P(None, GROUP_AXES), P(None, GROUP_AXES), P(GROUP_AXES, None), P(TOK_AXES, None, None, None))
    out_specs = (P(None, TOK_AXES, None), P(None, None, GROUP_AXES), P(TOK_AXES, None, None, None))
    return jax.shard_map(local_step, mesh=mesh, in_specs=in_specs, out_specs=out_specs, check_vma=False)
```

```python
import functools

import jax
import jax.numpy as jnp
from jax import lax
from jax.experimental import pallas as pl
from jax.experimental.pallas import tpu as pltpu
from jax.sharding import PartitionSpec as P

TOK_AXES = ("dp", "row", "fsdp")
GROUP_AXES = ("row", "fsdp")

D = 896
FF = 4864
N = 4096
SH = FF // 4
FT = 256
T = 1024
NF = FF // FT
TW = 512
NW = FF // TW
TL = FF - NW * TW
C = N // T
TP = 512
OS = 4
XS = 6
XB = 256
UN = 21
UR, UC = 128, 1280
A0, B0, C0, D0 = 6, 8, 11, 14
PS, QS = C0 - B0 + 1, D0 - C0 + 1
NT = (((1,), (1,)), ((), ()))
F32, BF16 = jnp.float32, jnp.bfloat16
MESH = pl.DeviceIdType.MESH


def step_kernel(x_h, dy_h, w1_h, w3_h, w2_h, g_h,
                dw_h, dx_h, dn_h, wg1, wg3, wg2, ra_h, rx_h, ry_h, db_h, hh_h, xt_h, dyt_h,
                xt, dyt, acc, wb, wn, dwb, gba, gbb, raw2, ob,
                ga, gb_in, sa, ra, pb, rx, qb, ry, tb,
                wsem, dsem, xsem, osem, lsem, agl, ags, agr,
                gas, gbs, ras, rxs, rys, tbs, gos, xos, sas, sar, sxs, sxr, sys_, syr):
    d = lax.axis_index("dp")
    r = lax.axis_index("row")
    c = lax.axis_index("fsdp")
    core = (d, r, 1 - c)
    xnb = (d, 1 - r, c)
    ynb = (1 - d, r, c)
    s = 2 * r + c
    so = 2 * (1 - r) + c

    bar = pltpu.get_barrier_semaphore()
    for dev in (core, xnb, ynb):
        pl.semaphore_signal(bar, inc=1, device_id=dev, device_id_type=MESH)
    pl.semaphore_wait(bar, 3)

    own = (w1_h, w3_h, w2_h)
    full = (wg1, wg3, wg2)

    def rows(start, size):
        return pl.ds(pl.multiple_of(start, 32), size)

    def remote(src, dst, ssem, rsem, dev):
        return pltpu.make_async_remote_copy(src_ref=src, dst_ref=dst, send_sem=ssem, recv_sem=rsem, device_id=dev, device_id_type=MESH)

    H = SH // 2

    def ag(kind, w):
        if kind == 0:
            return remote(own[w], full[w].at[rows(s * SH, SH)], ags.at[kind, w], agr.at[kind, w], core)
        if kind == 1:
            return remote(own[w].at[rows(d * H, H)], full[w].at[rows(s * SH + d * H, H)], ags.at[kind, w], agr.at[kind, w], xnb)
        got = full[w].at[rows(so * SH + d * H, H)]
        if kind == 2:
            return remote(got, got, ags.at[kind, w], agr.at[kind, w], ynb)
        if kind == 3:
            return remote(got, got, ags.at[kind, w], agr.at[kind, w], core)
        got = full[w].at[rows(so * SH + (1 - d) * H, H)]
        return remote(got, got, ags.at[kind, w], agr.at[kind, w], core)

    for w in range(3):
        ag(1, w).start()
    for w in range(3):
        ag(0, w).start()

    def edge(w, e):
        off = e * (SH - 192)
        return pltpu.make_async_copy(own[w].at[rows(off, 192)], full[w].at[rows(s * SH + off, 192)], agl.at[w, e])

    for w in range(3):
        for e in range(2):
            edge(w, e).start()

    def tile(j):
        one = jnp.where(j < 4, 5 + j, jnp.where(j < 9, 8 - j, jnp.where(j < 13, 6 + j, 27 - j)))
        zero = j
        t = jnp.where(r == c, zero, one)
        return jnp.where(r == 1, NF - 1 - t, t)

    def wcopy(j, slot, mine):
        t = tile(j)
        out = []
        for w in range(3):
            if mine:
                src = own[w].at[rows(t * FT - s * SH, FT)]
            else:
                src = full[w].at[rows(t * FT, FT)]
            out.append(pltpu.make_async_copy(src, wb.at[slot, pl.ds(w * FT, FT)], wsem.at[slot, w]))
        return out

    for cp in wcopy(0, 0, True):
        cp.start()
    for cp in wcopy(1, 1, True):
        cp.start()

    nx = N // XB

    def xload(k, act):
        sl = lax.rem(k, XS)
        rs = pl.ds(pl.multiple_of(lax.rem(k, nx) * XB, XB), XB)

        @pl.when(k < nx)
        def _():
            getattr(pltpu.make_async_copy(x_h.at[rs], ob.at[sl], xsem.at[sl]), act)()

        @pl.when(k >= nx)
        def _():
            getattr(pltpu.make_async_copy(dy_h.at[rs], ob.at[sl], xsem.at[sl]), act)()

    for k in range(XS - 1):
        xload(k, "start")

    def tr(k, _, dst=None):
        @pl.when(k + XS - 1 < 2 * nx)
        def _():
            xload(k + XS - 1, "start")
        xload(k, "wait")
        dst[:, pl.ds(pl.multiple_of(lax.rem(k, nx) * XB, XB), XB)] = ob[lax.rem(k, XS)].T
        return 0
    lax.fori_loop(0, nx, functools.partial(tr, dst=xt), 0)
    lax.fori_loop(nx, 2 * nx, functools.partial(tr, dst=dyt), 0)

    keep = (pltpu.make_async_copy(xt, xt_h, xos.at[0]), pltpu.make_async_copy(dyt, dyt_h, xos.at[1]))
    for cp in keep:
        cp.start()

    def zero(k, _):
        acc[:, pl.ds(pl.multiple_of(k * 256, 256), 256)] = jnp.zeros((D, 256), F32)
        return 0
    lax.fori_loop(0, N // 256, zero, 0)

    def trans(src, dst, k):
        ck = pl.ds(pl.multiple_of(k * 128, 128), 128)
        wn[dst, ck, 0:FT] = wb[src, 0:FT, ck].T
        wn[dst, ck, FT:2 * FT] = wb[src, FT:2 * FT, ck].T

    def products(it, raw):
        ck = lax.rem(it, C)
        ws = lax.rem(it // C, 3)

        def piece(half, p):
            to = pl.ds(p * TP, TP)
            cols = pl.ds(pl.multiple_of(ck * T + p * TP, TP), TP)
            if half == 0:
                raw[0:2 * FT, to] = jnp.dot(wb[ws, 0:2 * FT, :], xt[:, cols], preferred_element_type=F32)
            else:
                raw[2 * FT:3 * FT, to] = jnp.dot(wb[ws, 2 * FT:3 * FT, :], dyt[:, cols], preferred_element_type=F32)
        return [functools.partial(piece, half, p) for half in range(2) for p in range(T // TP)]

    def gates(raw, gb):
        def piece(i, p):
            to = pl.ds(p * 512, 512)
            a = raw[pl.ds(i * 16, 16), to]
            b = raw[pl.ds(FT + i * 16, 16), to]
            dh = raw[pl.ds(2 * FT + i * 16, 16), to]
            sg = jax.nn.sigmoid(a)
            act = a * sg
            gb[pl.ds(2 * FT + i * 16, 16), to] = (act * b).astype(BF16)
            gb[pl.ds(FT + i * 16, 16), to] = (dh * act).astype(BF16)
            gb[pl.ds(i * 16, 16), to] = ((dh * b) * (sg * (1.0 + (a - act)))).astype(BF16)
        return [functools.partial(piece, i, p) for p in range(T // 512) for i in range(FT // 16)]

    def add_dx(it, gb):
        ck = lax.rem(it, C)
        ns = lax.rem(it // C, 3)

        def piece(p):
            cols = pl.ds(pl.multiple_of(ck * T + p * TP, TP), TP)
            acc[:, cols] += jnp.dot(wn[ns], gb[0:2 * FT, p * TP:(p + 1) * TP], preferred_element_type=F32)
        return [functools.partial(piece, p) for p in range(T // TP)]

    def add_dw(it, gb):
        ck = lax.rem(it, C)
        ns = lax.rem(it // C, 2)
        cols = pl.ds(pl.multiple_of(ck * T, T), T)

        def piece(p):
            mr = pl.ds(p * (D // 2), D // 2)
            d0 = lax.dot_general(xt[mr, cols], gb[0:FT, :], NT, preferred_element_type=F32)
            dwb[ns, mr] = jnp.where(ck == 0, 0.0, dwb[ns, mr]) + d0
        return [functools.partial(piece, p) for p in range(2)]

    def dcopy(j):
        sl = lax.rem(j, 2)
        return pltpu.make_async_copy(dwb.at[sl], dw_h.at[:, pl.ds(pl.multiple_of(tile(j) * FT, 128), FT)], dsem.at[sl])

    def gcopy(it, gb, sl):
        rs = rows(tile(it // C) * FT, FT)
        cs = pl.ds(pl.multiple_of(lax.rem(it, C) * T, T), T)
        return [pltpu.make_async_copy(gb.at[pl.ds(FT, FT)], db_h.at[rs, cs], gos.at[sl, 0]),
                pltpu.make_async_copy(gb.at[pl.ds(2 * FT, FT)], hh_h.at[rs, cs], gos.at[sl, 1])]

    def ocopy(k):
        return pltpu.make_async_copy(ob.at[lax.rem(k, OS)], dx_h.at[pl.ds(pl.multiple_of(k * XB, XB), XB)], osem.at[lax.rem(k, OS)])

    def unit(u):
        return u // 7, lax.rem(u, 7)

    def gload(u, cc, buf, sem):
        k, i = unit(u)
        out = []
        for q in range(2):
            col = q * (FF // 2) + cc * 1152
            out.append(pltpu.make_async_copy(g_h.at[k, pl.ds(pl.multiple_of(i * UR, UR), UR), pl.ds(pl.multiple_of(col, 128), UC)], buf.at[q], sem.at[q]))
        return out

    def load_a(u):
        return gload(u, 1 - c, ga, gas)

    def load_b(u):
        return gload(u, c, gb_in, gbs) + [pltpu.make_async_copy(ra_h.at[u], ra, ras.at[0])]

    def send_a(u):
        return remote(sa.at[lax.rem(u, 2)], ra_h.at[u], sas.at[u], sar.at[u], core)

    def send_x(u):
        return remote(pb.at[lax.rem(u, PS), 1 - r], rx_h.at[u], sxs.at[u], sxr.at[u], xnb)

    def send_y(u):
        return remote(qb.at[lax.rem(u, QS)], ry_h.at[u], sys_.at[u], syr.at[u], ynb)

    def load_c(u):
        return pltpu.make_async_copy(rx_h.at[u], rx, rxs.at[0])

    def load_d(u):
        return pltpu.make_async_copy(ry_h.at[u], ry, rys.at[0])

    def out_d(u):
        sl = lax.rem(u, 2)
        return pltpu.make_async_copy(tb.at[sl, pl.ds(pl.multiple_of(64 * c, 64), SH)], dn_h.at[u // 7, :, pl.ds(pl.multiple_of(lax.rem(u, 7) * UR, UR), UR)], tbs.at[sl])

    def on(u):
        return (u >= 0) & (u < UN)

    def forward(it):
        for w in range(3):
            @pl.when(it == 6 + 6 * w)
            def _(w=w):
                ag(1, w).wait_recv()
                ag(2, w).start()
                ag(3, w).start()

            @pl.when(it == (14, 20, 28)[w])
            def _(w=w):
                ag(2, w).wait_recv()
                ag(4, w).start()

    def first_half(i):
        ua, ub, uc, ud = i - A0, i - B0, i - C0, i - D0

        @pl.when(on(uc - 1))
        def _():
            send_y(uc - 1).start()

        @pl.when(on(uc))
        def _():
            send_x(uc).wait_recv()
            load_c(uc).start()

        @pl.when(on(ud))
        def _():
            send_y(ud).wait_recv()
            load_d(ud).start()

        @pl.when(on(ua))
        def _():
            @pl.when(ua >= 2)
            def _():
                send_a(ua - 2).wait_send()
            for cp in load_a(ua):
                cp.wait()

        @pl.when(on(ub))
        def _():
            @pl.when(ub >= PS)
            def _():
                send_x(ub - PS).wait_send()
            for cp in load_b(ub):
                cp.wait()

    def second_half(i):
        ua, ub, uc, ud = i - A0, i - B0, i - C0, i - D0

        @pl.when(on(ua))
        def _():
            send_a(ua).start()

        @pl.when(on(ub))
        def _():
            send_x(ub).start()

        @pl.when(on(ua + 1))
        def _():
            for cp in load_a(ua + 1):
                cp.start()

        @pl.when(on(ub + 1))
        def _():
            send_a(ub + 1).wait_recv()
            for cp in load_b(ub + 1):
                cp.start()

        @pl.when(on(uc))
        def _():
            @pl.when(uc >= QS)
            def _():
                send_y(uc - QS).wait_send()
            load_c(uc).wait()

        @pl.when(on(ud))
        def _():
            @pl.when(ud >= 2)
            def _():
                out_d(ud - 2).wait()
            load_d(ud).wait()

    def mod(u, n):
        return lax.rem(u + 40 * n, n)

    def spot(u, n):
        return jnp.where(on(u), mod(u, n), n)

    def arith_ab(i):
        da, db = spot(i - A0, 2), spot(i - B0, PS)

        def cast(q, n):
            rs = pl.ds(n * 16, 16)
            sa[da, q, rs] = ga[q, rs].astype(BF16)

        def core_sum(q, n):
            rs = pl.ds(n * 16, 16)
            pb[db, q, rs] = gb_in[q, rs].astype(BF16) + ra[q, rs]
        return [functools.partial(f, q, n) for q in range(2) for n in range(UR // 16) for f in (cast, core_sum)]

    def arith_cd(i):
        uc, ud = i - C0, i - D0
        dc, dd = spot(uc, QS), spot(ud, 2)

        def row_sum(n):
            rs = pl.ds(n * 16, 16)
            qb[dc, rs] = pb[mod(uc, PS), r, rs] + rx[rs]

        def dp_sum(n):
            cs = pl.ds(n * 128, 128)
            tot = qb[mod(ud, QS), :, cs].astype(F32) + ry[:, cs].astype(F32)
            tb[dd, pl.ds(n * 128, 128), :] = tot.T
        return [functools.partial(dp_sum, n) for n in range(UC // 128)] + [functools.partial(row_sum, n) for n in range(UR // 16)]

    def flush(i):
        @pl.when(on(i - D0))
        def _():
            out_d(i - D0).start()

    for cp in wcopy(0, 0, True):
        cp.wait()
    for k in range(D // 128):
        trans(0, 0, k)
    for cp in wcopy(1, 1, True):
        cp.wait()
    for k in range(2):
        trans(1, 1, k)
    gbs2 = (gba, gbb)

    def body(it, par, step=None):
        j = it // C
        ck = lax.rem(it, C)
        jp = (it - 1) // C
        cp_ = lax.rem(it - 1, C)
        jn = j + 2

        @pl.when((ck == 1) & (jn < NF))
        def _():
            @pl.when(jn < 4)
            def _():
                for cp in wcopy(jn, lax.rem(jn, 3), True):
                    cp.start()

            @pl.when(jn >= 4)
            def _():
                @pl.when(jn == 4)
                def _():
                    for w in range(3):
                        for e in range(2):
                            edge(w, e).wait()
                        ag(0, w).wait_recv()

                @pl.when(jn == 9)
                def _():
                    for w in range(3):
                        ag(3, w).wait_recv()
                        ag(4, w).wait_recv()
                for cp in wcopy(jn, lax.rem(jn, 3), False):
                    cp.start()

        @pl.when((ck == 0) & (j + 1 < NF))
        def _():
            for cp in wcopy(j + 1, lax.rem(j + 1, 3), False):
                cp.wait()

        side = []
        if step is not None:
            if par == 0:
                forward(it)
                first_half(step)
                side = arith_ab(step)
            else:
                second_half(step)
                side = arith_cd(step)
        for cp in gcopy(it - 1, gbs2[1 - par], 1 - par):
            cp.start()

        @pl.when(it >= 2)
        def _():
            for cp in gcopy(it - 2, gbs2[par], par):
                cp.wait()

        @pl.when((cp_ == 0) & (jp >= 2))
        def _():
            dcopy(jp - 2).wait()
        prod, gate = products(it, raw2), gates(raw2, gbs2[par])
        grad = add_dx(it - 1, gbs2[1 - par]) + add_dw(it - 1, gbs2[1 - par])
        side += [functools.partial(trans, lax.rem(j + 1, 3), lax.rem(j + 1, 3), jnp.minimum(2 * ck + q, D // 128 - 1)) for q in range(2)]
        ng, nd = len(gate) // 2, len(side) // 2
        run(grad[2], prod[0], prod[2], *gate[:ng], grad[3], prod[1], prod[3], *side, *gate[ng:], grad[0], grad[1])
        if step is not None and par == 1:
            flush(step)
        grads_out(jp, cp_)

    def run(*fs):
        for f in fs:
            f()

    def grads_out(jp, cp_):
        @pl.when(cp_ == C - 1)
        def _():
            dcopy(jp).start()

        @pl.when(jp == NF - 1)
        def _():
            for q in range(T // XB):
                k = cp_ * (T // XB) + q

                @pl.when(k >= OS)
                def _():
                    ocopy(k - OS).wait()
                ob[q % OS] = acc[:, pl.ds(pl.multiple_of(k * XB, XB), XB)].astype(BF16).T
                ocopy(k).start()

    run(*products(0, raw2), *gates(raw2, gba))
    body(1, 1)

    def pair(i, _):
        body(2 * i + 2, 0, i)
        body(2 * i + 3, 1, i)
        return 0
    lax.fori_loop(0, NF * C // 2 - 1, pair, 0)
    last = NF * C - 1
    for cp in gcopy(last, gbb, 1):
        cp.start()
    for cp in gcopy(last - 1, gba, 0):
        cp.wait()
    run(*add_dx(last, gbb), *add_dw(last, gbb))
    grads_out(NF - 1, C - 1)

    dcopy(NF - 2).wait()
    dcopy(NF - 1).wait()
    for cp in gcopy(NF * C - 1, gbb, 1):
        cp.wait()
    for cp in keep:
        cp.wait()
    for k in range(OS):
        ocopy(N // XB - OS + k).wait()
    out_d(19).wait()
    out_d(20).wait()
    for w in range(3):
        for kind in range(5):
            ag(kind, w).wait_send()
    for u in range(UN - 2, UN):
        send_a(u).wait_send()
    for u in range(UN - PS, UN):
        send_x(u).wait_send()
    for u in range(UN - QS, UN):
        send_y(u).wait_send()


def tail_kernel(xt_h, dyt_h, db_h, hh_h, d0_h, dxi_h, dni_h, dw_h, dx_h, dn_h,
                xt, dyt, db, hh, ow, bx, bn, xsem, gsem, osem, dsem, bsem, csem):
    def part(j, width):
        return pl.ds(pl.multiple_of(j * TW, TW), width)

    def loads(j, width):
        sl = lax.rem(j, 2)
        to = pl.ds(0, width)
        return [pltpu.make_async_copy(db_h.at[part(j, width)], db.at[sl, to], gsem.at[sl, 0]),
                pltpu.make_async_copy(hh_h.at[part(j, width)], hh.at[sl, to], gsem.at[sl, 1])]

    def slab0(j, width):
        sl = lax.rem(j, 2)
        return pltpu.make_async_copy(d0_h.at[:, part(j, width)], ow.at[sl, 0, :, pl.ds(0, width)], dsem.at[sl])

    def out(j, width):
        sl = lax.rem(j, 2)
        return pltpu.make_async_copy(ow.at[sl, :, :, pl.ds(0, width)], dw_h.at[:, :, part(j, width)], osem.at[sl])

    def carry(j, put):
        sl = lax.rem(j, 2)
        rx = pl.ds(pl.multiple_of(j * (N // 8), 128), N // 8)
        rn = pl.ds(pl.multiple_of(j * (SH // 8), 8), SH // 8)
        if put:
            return (pltpu.make_async_copy(bx.at[sl], dx_h.at[rx], csem.at[sl, 0]),
                    pltpu.make_async_copy(bn.at[sl], dn_h.at[:, rn], csem.at[sl, 1]))
        return (pltpu.make_async_copy(dxi_h.at[rx], bx.at[sl], bsem.at[sl, 0]),
                pltpu.make_async_copy(dni_h.at[:, rn], bn.at[sl], bsem.at[sl, 1]))

    ldx = pltpu.make_async_copy(xt_h, xt, xsem.at[0])
    ldy = pltpu.make_async_copy(dyt_h, dyt, xsem.at[1])
    first = loads(0, TW)
    first[0].start()
    ldx.start()
    first[1].start()
    ldy.start()
    slab0(0, TW).start()
    for cp in carry(0, False):
        cp.start()

    def step(j, _):
        sl = lax.rem(j, 2)

        @pl.when(j == 0)
        def _():
            ldx.wait()

        @pl.when((j >= 1) & (j <= 8))
        def _():
            for cp in carry(j - 1, False):
                cp.wait()
            for cp in carry(j - 1, True):
                cp.start()

        @pl.when(j < NW - 1)
        def _():
            for cp in loads(j + 1, TW):
                cp.start()

        @pl.when(j == NW - 1)
        def _():
            for cp in loads(j + 1, TL):
                cp.start()
        loads(j, TW)[0].wait()
        ow[sl, 1] = lax.dot_general(xt[...], db[sl], NT, preferred_element_type=F32)

        @pl.when(j == 0)
        def _():
            ldy.wait()
        loads(j, TW)[1].wait()

        @pl.when(j >= 1)
        def _():
            out(j - 1, TW).wait()
            for cp in carry(j - 1, True):
                cp.wait()

        @pl.when(j < NW - 1)
        def _():
            slab0(j + 1, TW).start()

        @pl.when(j == NW - 1)
        def _():
            slab0(j + 1, TL).start()

        @pl.when(j + 1 < 8)
        def _():
            for cp in carry(j + 1, False):
                cp.start()
        ow[sl, 2] = lax.dot_general(dyt[...], hh[sl], NT, preferred_element_type=F32)
        slab0(j, TW).wait()
        out(j, TW).start()
        return 0
    lax.fori_loop(0, NW, step, 0)

    for cp in loads(NW, TL):
        cp.wait()
    sl = NW % 2
    for p in range(2):
        mr = pl.ds(p * (D // 2), D // 2)
        ow[sl, 1, mr, 0:TL] = lax.dot_general(xt[mr], db[sl, 0:TL], NT, preferred_element_type=F32)
        ow[sl, 2, mr, 0:TL] = lax.dot_general(dyt[mr], hh[sl, 0:TL], NT, preferred_element_type=F32)
    slab0(NW, TL).wait()
    out(NW, TL).start()
    out(NW - 1, TW).wait()
    out(NW, TL).wait()


def solution(mesh):
    def local_step(x_dev, dy_dev, gate_shard, up_shard, down_shard, g_dev):
        any_spec = pl.BlockSpec(memory_space=pl.ANY)
        sds = jax.ShapeDtypeStruct
        dma = pltpu.SemaphoreType.DMA
        vm = pltpu.VMEM
        outs = pl.pallas_call(
            step_kernel,
            in_specs=[any_spec] * 6,
            out_specs=[any_spec] * 13,
            out_shape=[sds((D, FF), F32), sds((N, D), BF16), sds((3, SH, D), F32),
                       sds((FF, D), BF16), sds((FF, D), BF16), sds((FF, D), BF16),
                       sds((UN, 2, UR, UC), BF16), sds((UN, UR, UC), BF16), sds((UN, UR, UC), BF16),
                       sds((FF, N), BF16), sds((FF, N), BF16), sds((D, N), BF16), sds((D, N), BF16)],
            scratch_shapes=[
                vm((D, N), BF16), vm((D, N), BF16), vm((D, N), F32),
                vm((3, 3 * FT, D), BF16), vm((3, D, 2 * FT), BF16), vm((2, D, FT), F32),
                vm((3 * FT, T), BF16), vm((3 * FT, T), BF16), vm((3 * FT, T), F32), vm((XS, XB, D), BF16),
                vm((2, UR, UC), F32), vm((2, UR, UC), F32), vm((3, 2, UR, UC), BF16),
                vm((2, UR, UC), BF16), vm((PS + 1, 2, UR, UC), BF16), vm((UR, UC), BF16),
                vm((QS + 1, UR, UC), BF16), vm((UR, UC), BF16), vm((3, UC, UR), F32),
                dma((3, 3)), dma((2,)), dma((XS,)), dma((OS,)), dma((1,)), dma((3, 2)), dma((5, 3)), dma((5, 3)),
                dma((2,)), dma((2,)), dma((1,)), dma((1,)), dma((1,)), dma((2,)), dma((2, 2)), dma((2,)),
                dma((UN,)), dma((UN,)), dma((UN,)), dma((UN,)), dma((UN,)), dma((UN,)),
            ],
            compiler_params=pltpu.CompilerParams(collective_id=0, has_side_effects=True, vmem_limit_bytes=65470 * 1024),
        )(x_dev.reshape(N, D), dy_dev.reshape(N, D), gate_shard.T, up_shard.T, down_shard, g_dev[0])
        dw, dx, dn = pl.pallas_call(
            tail_kernel,
            in_specs=[any_spec] * 7,
            out_specs=[any_spec] * 3,
            out_shape=[sds((3, D, FF), F32), sds((N, D), BF16), sds((3, SH, D), F32)],
            scratch_shapes=[
                vm((D, N), BF16), vm((D, N), BF16), vm((2, TW, N), BF16), vm((2, TW, N), BF16), vm((2, 3, D, TW), F32),
                vm((2, N // 8, D), BF16), vm((2, 3, SH // 8, D), F32),
                dma((2,)), dma((2, 2)), dma((2,)), dma((2,)), dma((2, 2)), dma((2, 2)),
            ],
            compiler_params=pltpu.CompilerParams(vmem_limit_bytes=60 * 1024 * 1024),
        )(outs[11], outs[12], outs[9], outs[10], outs[0], outs[1], outs[2])
        return dx.reshape(2, N // 2, D), dn.transpose(0, 2, 1), dw[None]

    in_specs = (P(None, TOK_AXES, None), P(None, TOK_AXES, None), P(None, GROUP_AXES), P(None, GROUP_AXES), P(GROUP_AXES, None), P(TOK_AXES, None, None, None))
    out_specs = (P(None, TOK_AXES, None), P(None, None, GROUP_AXES), P(TOK_AXES, None, None, None))
    return jax.shard_map(local_step, mesh=mesh, in_specs=in_specs, out_specs=out_specs, check_vma=False)
```
